512 devices in a mesh: ep: 128 (over x, z, core), rep: 4 (over y).
Axes of the slice: x: 4, y: 4, z: 16, core: 2. Of those that a mesh axis runs over, the one named last changes fastest.
Arguments:
- tension: float32 [65536, 512], P(('rep', 'ep')), parts along dimension 0, may hold values from -6 to 6
- tile_dest: int32 [65536], P(('rep', 'ep')), parts along dimension 0, may hold values from 0 to 16383, as said below
- restriction: float32 [8, 64], replicated, may hold values from -0.75 to 0.75
- elem_block: int32 [524288], P(('rep', 'ep')), parts along dimension 0, may hold values from 0 to 1023
- shared_own: int32 [131072], P(('rep', 'ep')), parts along dimension 0, may hold values from 0 to 1023, as said below
- shared_send: int32 [131072], P(('rep', 'ep')), parts along dimension 0, may hold values from 0 to 1023
Outputs:
- quadrature: float32 [8, 524288], P(None, ('rep', 'ep')), parts along dimension 1
The draws below stay inside these ranges and needn't reach their ends.
There are 4 independent parts, one for each index of `rep`. The reference program is written for one: setup_inputs(seed, part) draws one part's arguments, and reference() takes and returns one part's arrays. A program takes and returns all parts, laid end to end along the dimension named above; an argument that names none is the same for every part. Nothing has to cross between parts.
Inputs may be any that keep to these rules, and one draw needn't show every extreme that they name: `tile_dest`: A permutation of the tile positions. The 128 entries of one device name, for each device's block of 128 positions, either exactly 2 positions in it or none. `shared_own`: the 256 entries of one device are distinct.
All inputs are finite; a program needn't handle non-finite values.
Results may differ from the reference program's by a relative error of at most 0.00007.
Values sent between devices are 32-bit elements; how exact they have to be, the bound alone decides.
No kernel may reach another device: no remote copies, remote signals or barrier semaphores. Data moves between devices by JAX's collectives and lax.ppermute only.
A program may use at most 64 MiB of HBM per device.

```python
import jax
import jax.numpy as jnp
from jax import lax

TILE_NODES = 512
ELEM_NODES = 64
QUAD = 8
TILE_DEV = 128
SHARED = 256
BLOCKS = 8
CAP = 2
TILES = 16384
ELEM_DEV = 1024
ELEMENTS = 131072
N_EP = 128


def draw_tile_dest(key, part):
    key_one, key_two, key_three, key_four = jax.random.split(key, 4)
    sigma = jax.random.permutation(key_one, N_EP).astype(jnp.int32)
    tau = jax.random.permutation(key_two, N_EP).astype(jnp.int32)
    linked = ((sigma[:, None] + tau[None, :]) % 2 == 0).astype(jnp.int32)
    half_ep = N_EP // 2
    chosen = jnp.argsort(1 - linked, axis=1, stable=True)[:, :half_ep].astype(jnp.int32)
    offsets = (jnp.cumsum(linked, axis=0) - linked) * CAP
    slot_ids = jnp.arange(TILE_DEV, dtype=jnp.int32)
    dst_of = chosen[:, slot_ids // CAP]
    local_pos = jnp.take_along_axis(offsets, dst_of, axis=1) + (slot_ids % CAP)[None, :]
    shuffle_dst = jax.vmap(lambda sub: jax.random.permutation(sub, TILE_DEV))(jax.random.split(key_three, N_EP)).astype(jnp.int32)
    final_pos = shuffle_dst[dst_of, local_pos]
    global_dest = dst_of * TILE_DEV + final_pos
    shuffle_src = jax.vmap(lambda sub: jax.random.permutation(sub, TILE_DEV))(jax.random.split(key_four, N_EP)).astype(jnp.int32)
    dest = jnp.take_along_axis(global_dest, shuffle_src, axis=1)
    return dest.reshape(TILES).astype(jnp.int32)


def draw_shared_own(key, part):
    orders = jax.vmap(lambda sub: jax.random.permutation(sub, ELEM_DEV))(jax.random.split(jax.random.fold_in(key, 7), N_EP))
    return orders[:, :SHARED].reshape(N_EP * SHARED).astype(jnp.int32)


def touch_ends(entries, own_key, least, top_value):
    longest = entries.shape.index(max(entries.shape))
    spots = []
    for shift in (0, 1):
        where = [jax.random.randint(jax.random.fold_in(own_key, axis), (), 0, length) for axis, length in enumerate(entries.shape)]
        where[longest] = (where[longest] + shift) % entries.shape[longest]
        spots.append(tuple(where))
    return entries.at[spots[0]].set(least).at[spots[1]].set(top_value)


def block_scale(key, extent, pieces, low, largest):
    level = 1.0
    for dim, parts in pieces:
        heights = jax.random.uniform(jax.random.fold_in(jax.random.fold_in(key, 6), dim), (parts,), jnp.float32, low / len(pieces), largest / len(pieces))
        level = level * jnp.repeat(jnp.exp(heights), extent[dim] // parts).reshape((-1,) + (1,) * (len(extent) - 1 - dim))
    return level


def centred(key, extent, width, reach, cuts=(), held_as=jnp.bfloat16):
    factor_of = block_scale(key, extent, cuts, -0.22, 0.18) if cuts else 1.0
    values = jax.random.normal(key, extent, jnp.float32) * width * factor_of
    return jnp.minimum(jnp.maximum(values, -reach), reach).astype(held_as)


def setup_inputs(seed: int = 0, part: int = 0) -> dict:
    arg_keys = jax.random.split(jax.random.key(seed), 7)
    part_keys = jax.random.split(jax.random.fold_in(arg_keys[6], part), 7)
    tension = centred(part_keys[0], (TILES, TILE_NODES), 1.0, 6.0, ((0, 128),), jnp.float32)
    tile_dest = draw_tile_dest(jax.random.fold_in(jax.random.fold_in(arg_keys[6], part), 71), part)
    restriction = centred(arg_keys[2], (QUAD, ELEM_NODES), ELEM_NODES ** -0.5, 0.75, (), jnp.float32)
    elem_block = touch_ends(jax.random.randint(part_keys[3], (ELEMENTS,), 0, ELEM_DEV), jax.random.fold_in(part_keys[3], 1), 0, ELEM_DEV - 1).astype(jnp.int32)
    shared_own = draw_shared_own(jax.random.fold_in(jax.random.fold_in(arg_keys[6], part), 71), part)
    shared_send = touch_ends(jax.random.randint(part_keys[5], (N_EP * SHARED,), 0, ELEM_DEV), jax.random.fold_in(part_keys[5], 1), 0, ELEM_DEV - 1).astype(jnp.int32)
    return {"tension": tension, "tile_dest": tile_dest, "restriction": restriction, "elem_block": elem_block, "shared_own": shared_own, "shared_send": shared_send}


def reference(tension, tile_dest, restriction, elem_block, shared_own, shared_send):
    placed = jnp.zeros_like(tension).at[tile_dest].set(tension)
    blocks = placed.reshape(TILES * BLOCKS, ELEM_NODES)
    owner_dev = jnp.arange(ELEMENTS, dtype=jnp.int32) // ELEM_DEV
    source = (owner_dev * ELEM_DEV + elem_block).astype(jnp.int32)
    quad_values = jnp.dot(blocks[source], restriction.T, precision=lax.Precision.HIGHEST, preferred_element_type=jnp.float32)
    device = jnp.arange(N_EP * SHARED, dtype=jnp.int32) // SHARED
    next_dev = (device + 1) % N_EP
    next_send = jnp.roll(shared_send, -SHARED)
    own_rows = (device * ELEM_DEV + shared_own).astype(jnp.int32)
    ghost_rows = (next_dev * ELEM_DEV + next_send).astype(jnp.int32)
    mixed = 0.5 * (quad_values[own_rows] + quad_values[ghost_rows])
    averaged = quad_values.at[own_rows].set(mixed)
    return averaged.T
```

```python
import jax
import jax.numpy as jnp
from jax import lax
from jax.experimental import pallas as pl
from jax.experimental.pallas import tpu as pltpu
from jax.sharding import Mesh
from jax.sharding import PartitionSpec as P

LANES = 128
TILE_DEV = 128
ELEM_DEV = 1024
SHARED = 256
BLOCKS = 8
QUAD = 8
WIDTH = BLOCKS * QUAD
CHIPS = 64
ROWS = 4


def iota(shape, dim):
    return lax.broadcasted_iota(jnp.int32, shape, dim)


def split3(x):
    high = x.astype(jnp.bfloat16)
    rest = x - high.astype(jnp.float32)
    mid = rest.astype(jnp.bfloat16)
    low = (rest - mid.astype(jnp.float32)).astype(jnp.bfloat16)
    return high, mid, low


def dot(a, b, contract, **kw):
    return lax.dot_general(a, b, ((contract[:1], contract[1:]), ((), ())), preferred_element_type=jnp.float32, **kw)


def pack_kernel(tension_ref, dest_ref, restriction_ref, out_ref):
    wide = jnp.concatenate([restriction_ref[...]] * BLOCKS, axis=1)
    block = iota(wide.shape, 1) // (wide.shape[1] // BLOCKS)
    weight = jnp.concatenate([jnp.where(block == b, wide, 0.0) for b in range(BLOCKS)], axis=0)
    quad = dot(tension_ref[...], weight, (1, 1), precision=lax.Precision.HIGHEST)
    dest = dest_ref[...]
    target = dest // TILE_DEV
    position = (dest % TILE_DEV).astype(jnp.float32)
    shape = (2 * CHIPS, TILE_DEV)
    row, lane = iota(shape, 0), iota(shape, 1)
    owner = jnp.where(row < CHIPS, 2 * row, 2 * row - (2 * CHIPS - 1))
    hit = jnp.broadcast_to(target, shape) == owner
    lane_f = lane.astype(jnp.float32)
    first = jnp.min(jnp.where(hit, lane_f, float(TILE_DEV)), axis=1, keepdims=True)
    one = lane_f == first
    two = jnp.logical_and(hit, lane_f != first)
    spread = jnp.broadcast_to(position, shape)
    where_one = jnp.max(jnp.where(one, spread, -1.0), axis=1, keepdims=True)
    where_two = jnp.max(jnp.where(two, spread, -1.0), axis=1, keepdims=True)
    pick = jnp.concatenate(
        [jnp.where(one, 1.0, 0.0).astype(jnp.bfloat16), jnp.where(two, 1.0, 0.0).astype(jnp.bfloat16)], axis=1
    )
    data = jnp.zeros(shape, jnp.float32)
    for part in split3(quad):
        nil = jnp.zeros_like(part)
        both = jnp.concatenate(
            [jnp.concatenate([part, nil], axis=1), jnp.concatenate([nil, part], axis=1)], axis=0
        )
        data = data + dot(pick, both, (1, 0))
    even, odd = data[:CHIPS], data[CHIPS:]

    def ahead(x):
        return jnp.concatenate([x[1:], x[:1]], axis=0)

    column = lane[:CHIPS]
    places = jnp.zeros((CHIPS, LANES), jnp.float32)
    firsts, seconds = where_one[:CHIPS], where_two[:CHIPS]
    columns = (firsts, seconds, where_one[CHIPS:], where_two[CHIPS:], ahead(firsts), ahead(seconds))
    for i, value in enumerate(columns):
        places = jnp.where(column == i, jnp.broadcast_to(value, places.shape), places)
    for i, value in enumerate((even, odd, ahead(even), places)):
        out_ref[pl.ds(i, CHIPS, stride=ROWS), :] = value


def send_index_kernel(block_ref, send_ref, _, out_ref):
    block = block_ref[...]
    row = iota((QUAD, ELEM_DEV), 0)
    wide = jnp.broadcast_to(block, row.shape)
    left = jnp.where(row == 0, wide // BLOCKS, jnp.where(row == 1, wide % BLOCKS, 0))
    shape = (ELEM_DEV, SHARED)
    pick = jnp.where(iota(shape, 0) == jnp.broadcast_to(send_ref[...], shape), 1.0, 0.0)
    out_ref[...] = dot(left.astype(jnp.float32).astype(jnp.bfloat16), pick.astype(jnp.bfloat16), (1, 0))


def own_index_kernel(index_ref, own_ref, out_ref):
    index = index_ref[...]
    row = iota(index.shape, 0)
    left = jnp.where(row == 2, 1.0, index)
    shape = (ELEM_DEV, SHARED)
    pick = jnp.where(iota(shape, 0) == jnp.broadcast_to(own_ref[...], shape), 1.0, 0.0)
    placed = dot(left.astype(jnp.bfloat16), pick.astype(jnp.bfloat16), (1, 1))
    shared = placed[2:3] > 0.5
    out_ref[...] = jnp.where(iota(placed.shape, 0) == 0, jnp.where(shared, placed, -1.0), placed)


def gather(table, places, tile, block):
    turned = table.T
    left = jnp.concatenate(
        [jnp.concatenate([part[:WIDTH], part[WIDTH:]], axis=1) for part in split3(turned)], axis=0
    )
    shape = (TILE_DEV, tile.shape[1])
    wide = jnp.broadcast_to(tile, shape)
    pick = jnp.concatenate(
        [jnp.where(jnp.broadcast_to(place, shape) == wide, 1.0, 0.0).astype(jnp.bfloat16) for place in places], axis=0
    )
    tall = dot(left, pick, (1, 0))
    tall = tall[:WIDTH] + tall[WIDTH : 2 * WIDTH] + tall[2 * WIDTH :]
    which = jnp.broadcast_to(block, (QUAD, tile.shape[1]))
    out = jnp.zeros(which.shape, jnp.float32)
    for b in range(BLOCKS):
        out = jnp.where(which == float(b), tall[b * QUAD : (b + 1) * QUAD], out)
    return out


def place_kernel(core_ref, inbox_ref, block_ref, ghost_ref, out_ref):
    even_core = core_ref[0] == 0
    rows = [inbox_ref[pl.ds(i, 2 * CHIPS, stride=ROWS), :] for i in range(ROWS)]
    own = jnp.where(even_core, rows[0], rows[1])
    following = jnp.where(even_core, rows[1], rows[2])
    places = jnp.where(even_core, rows[3], pltpu.roll(rows[3], LANES - 2, 1))
    block = block_ref[...]
    mine = gather(
        own,
        (places[:, 0:1], places[:, 1:2]),
        (block // BLOCKS).astype(jnp.float32),
        (block % BLOCKS).astype(jnp.float32),
    )
    tile = ghost_ref[0:1, :]
    ghost = gather(following, (places[:, 2:3], places[:, 3:4]), tile, ghost_ref[1:2, :])
    shared = jnp.broadcast_to(tile, ghost.shape) >= 0.0
    out_ref[...] = jnp.where(shared, 0.5 * (mine + ghost), mine)


def call(kernel, shape, scalar=False):
    kw = {}
    return pl.pallas_call(
        kernel,
        out_shape=jax.ShapeDtypeStruct(shape, jnp.float32),
        name=kernel.__name__,
        **kw,
    )


def per_device(tension, tile_dest, restriction, elem_block, shared_own, shared_send):
    core = lax.axis_index("core").reshape(1)
    outbox = call(pack_kernel, (CHIPS * ROWS, LANES))(tension, tile_dest.reshape(1, -1), restriction)
    inbox = lax.all_to_all(outbox.reshape(CHIPS, ROWS, LANES), "chip", 0, 0, tiled=True)
    index = call(send_index_kernel, (QUAD, SHARED))(
        elem_block.reshape(1, -1), shared_send.reshape(1, -1), outbox[:8]
    )
    count = 2 * CHIPS
    index = lax.ppermute(index, ("chip", "core"), [(i, (i - 1) % count) for i in range(count)])
    ghost = call(own_index_kernel, (QUAD, ELEM_DEV))(index, shared_own.reshape(1, -1))
    inbox = lax.all_gather(inbox.reshape(CHIPS * ROWS, LANES), "core", tiled=True)
    return pl.pallas_call(
        place_kernel,
        out_shape=jax.ShapeDtypeStruct((QUAD, ELEM_DEV), jnp.float32),
        in_specs=[pl.BlockSpec(memory_space=pltpu.SMEM)] + [pl.BlockSpec(memory_space=pltpu.VMEM)] * 3,
        name="place_kernel",
    )(core, inbox, elem_block.reshape(1, -1), ghost)


def solution(mesh):
    split = Mesh(mesh.devices.reshape(CHIPS, 2, -1), ("chip", "core", "rep"))
    spread = P(("rep", "chip", "core"))
    return jax.shard_map(
        per_device,
        mesh=split,
        in_specs=(spread, spread, P(), spread, spread, spread),
        out_specs=P(None, ("rep", "chip", "core")),
        check_vma=False,
    )
```

```python
import jax
import jax.numpy as jnp
from jax import lax
from jax.experimental import pallas as pl
from jax.experimental.pallas import tpu as pltpu
from jax.sharding import Mesh
from jax.sharding import PartitionSpec as P

LANES = 128
TILE_DEV = 128
ELEM_DEV = 1024
SHARED = 256
BLOCKS = 8
QUAD = 8
WIDTH = BLOCKS * QUAD
CHIPS = 64
ROWS = 4


def iota(shape, dim):
    return lax.broadcasted_iota(jnp.int32, shape, dim)


def split3(x):
    high = x.astype(jnp.bfloat16)
    rest = x - high.astype(jnp.float32)
    mid = rest.astype(jnp.bfloat16)
    low = (rest - mid.astype(jnp.float32)).astype(jnp.bfloat16)
    return high, mid, low


def dot(a, b, contract, **kw):
    return lax.dot_general(a, b, ((contract[:1], contract[1:]), ((), ())), preferred_element_type=jnp.float32, **kw)


def pack_kernel(tension_any, dest_any, restriction_any, out_ref, token_ref, tension_ref, dest_ref, restriction_ref, sems):
    pairs = ((restriction_any, restriction_ref), (dest_any, dest_ref), (tension_any, tension_ref))
    copies = [pltpu.make_async_copy(a, b, sems.at[i]) for i, (a, b) in enumerate(pairs)]
    for copy in copies:
        copy.start()
    copies[0].wait()
    wide = jnp.concatenate([restriction_ref[...]] * BLOCKS, axis=1)
    block = iota(wide.shape, 1) // (wide.shape[1] // BLOCKS)
    weight = jnp.concatenate([jnp.where(block == b, wide, 0.0) for b in range(BLOCKS)], axis=0)
    copies[1].wait()
    dest = dest_ref[...]
    target = dest >> 7
    position = (dest & (TILE_DEV - 1)).astype(jnp.float32)
    shape = (2 * CHIPS, TILE_DEV)
    row, lane = iota(shape, 0), iota(shape, 1)
    owner = jnp.where(row < CHIPS, 2 * row, 2 * row - (2 * CHIPS - 1))
    hit = jnp.broadcast_to(target, shape) == owner
    lane_f = lane.astype(jnp.float32)
    first = jnp.min(jnp.where(hit, lane_f, float(TILE_DEV)), axis=1, keepdims=True)
    one = lane_f == first
    two = jnp.logical_and(hit, lane_f != first)
    spread = jnp.broadcast_to(position, shape)
    where_one = jnp.max(jnp.where(one, spread, -1.0), axis=1, keepdims=True)
    where_two = jnp.max(jnp.where(two, spread, -1.0), axis=1, keepdims=True)
    pick = jnp.concatenate(
        [jnp.where(one, 1.0, 0.0).astype(jnp.bfloat16), jnp.where(two, 1.0, 0.0).astype(jnp.bfloat16)], axis=1
    )
    copies[2].wait()
    quad = dot(tension_ref[...], weight, (1, 1), precision=lax.Precision.HIGHEST)
    data = jnp.zeros(shape, jnp.float32)
    for part in split3(quad):
        nil = jnp.zeros_like(part)
        both = jnp.concatenate(
            [jnp.concatenate([part, nil], axis=1), jnp.concatenate([nil, part], axis=1)], axis=0
        )
        data = data + dot(pick, both, (1, 0))
    even, odd = data[:CHIPS], data[CHIPS:]

    def ahead(x):
        return jnp.concatenate([x[1:], x[:1]], axis=0)

    column = lane[:CHIPS]
    places = jnp.zeros((CHIPS, LANES), jnp.float32)
    firsts, seconds = where_one[:CHIPS], where_two[:CHIPS]
    columns = (firsts, seconds, where_one[CHIPS:], where_two[CHIPS:], ahead(firsts), ahead(seconds))
    for i, value in enumerate(columns):
        places = jnp.where(column == i, jnp.broadcast_to(value, places.shape), places)
    token_ref[...] = places[:8]
    for i, value in enumerate((even, odd, ahead(even), places)):
        out_ref[pl.ds(i, CHIPS, stride=ROWS), :] = value


def send_index_kernel(block_ref, send_ref, _, out_ref):
    block = block_ref[...]
    left = jnp.concatenate([block >> 3, block & 7], axis=0).astype(jnp.float32).astype(jnp.bfloat16)
    send = send_ref[...]
    shape = (LANES, SHARED)
    pick = jnp.where(iota(shape, 0) == jnp.broadcast_to(send & (LANES - 1), shape), 1.0, 0.0)
    rows = dot(left, pick.astype(jnp.bfloat16), (1, 0))
    shape = (ELEM_DEV // LANES, SHARED)
    high = iota(shape, 0) == jnp.broadcast_to(send >> 7, shape)
    tile = jnp.sum(jnp.where(high, rows[: shape[0]], 0.0), axis=0, keepdims=True)
    block = jnp.sum(jnp.where(high, rows[shape[0] :], 0.0), axis=0, keepdims=True)
    row = iota((QUAD, SHARED), 0)
    out_ref[...] = jnp.where(row == 0, jnp.broadcast_to(tile, row.shape), jnp.broadcast_to(block, row.shape))


def own_index_kernel(index_ref, own_ref, tile_ref, block_ref):
    own = own_ref[...]
    shape = (ELEM_DEV // LANES, SHARED)
    high = iota(shape, 0) == jnp.broadcast_to(own >> 7, shape)
    rows = [index_ref[0:1, :] + 1.0, index_ref[1:2, :]]
    left = jnp.concatenate([jnp.where(high, jnp.broadcast_to(row, shape), 0.0) for row in rows], axis=0)
    wide = (LANES, SHARED)
    pick = jnp.where(iota(wide, 0) == jnp.broadcast_to(own & (LANES - 1), wide), 1.0, 0.0)
    placed = dot(left.astype(jnp.bfloat16), pick.astype(jnp.bfloat16), (1, 1))
    tile_ref[...] = placed[: shape[0]] - 1.0
    block_ref[...] = placed[shape[0] :]


def gather(table, places, tile, block):
    turned = table.T
    left = jnp.concatenate(
        [jnp.concatenate([part[:WIDTH], part[WIDTH:]], axis=1) for part in split3(turned)], axis=0
    )
    shape = (TILE_DEV, tile.shape[1])
    wide = jnp.broadcast_to(tile, shape)
    pick = jnp.concatenate(
        [jnp.where(jnp.broadcast_to(place, shape) == wide, 1.0, 0.0).astype(jnp.bfloat16) for place in places], axis=0
    )
    tall = dot(left, pick, (1, 0))
    tall = tall[:WIDTH] + tall[WIDTH : 2 * WIDTH] + tall[2 * WIDTH :]
    which = jnp.broadcast_to(block, (QUAD, tile.shape[1]))
    out = jnp.zeros(which.shape, jnp.float32)
    for b in range(BLOCKS):
        out = jnp.where(which == float(b), tall[b * QUAD : (b + 1) * QUAD], out)
    return out


def place_kernel(core_ref, inbox_ref, block_ref, tile_ref, ghost_block_ref, out_ref):
    even_core = core_ref[0] == 0
    rows = [inbox_ref[pl.ds(i, 2 * CHIPS, stride=ROWS), :] for i in range(ROWS)]
    own = jnp.where(even_core, rows[0], rows[1])
    following = jnp.where(even_core, rows[1], rows[2])
    places = jnp.where(even_core, rows[3], pltpu.roll(rows[3], LANES - 2, 1))
    block = block_ref[...]
    mine = gather(
        own,
        (places[:, 0:1], places[:, 1:2]),
        (block >> 3).astype(jnp.float32),
        (block & 7).astype(jnp.float32),
    )
    tile = tile_ref[...]
    ghost = gather(following, (places[:, 2:3], places[:, 3:4]), tile, ghost_block_ref[...])
    shared = jnp.broadcast_to(tile, ghost.shape) >= 0.0
    out_ref[...] = jnp.where(shared, 0.5 * (mine + ghost), mine)


def call(kernel, shapes, spaces, scratch=(), limit=4):
    return pl.pallas_call(
        kernel,
        out_shape=jax.tree.map(lambda s: jax.ShapeDtypeStruct(s, jnp.float32), shapes, is_leaf=lambda s: isinstance(s[0], int)),
        in_specs=[pl.BlockSpec(memory_space=space) for space in spaces],
        scratch_shapes=scratch,
        compiler_params=pltpu.CompilerParams(vmem_limit_bytes=limit << 20),
        name=kernel.__name__,
    )


def per_device(tension, tile_dest, restriction, elem_block, shared_own, shared_send):
    V, S = pltpu.VMEM, pltpu.SMEM
    core = lax.axis_index("core").reshape(1)
    inputs = (tension, tile_dest.reshape(1, -1), restriction)
    scratch = [V(x.shape, x.dtype) for x in inputs] + [pltpu.SemaphoreType.DMA((3,))]
    outbox, token = call(pack_kernel, ((CHIPS * ROWS, LANES), (8, LANES)), [pl.ANY] * 3, scratch, 60)(*inputs)
    inbox = lax.all_to_all(outbox.reshape(CHIPS, ROWS, LANES), "chip", 0, 0, tiled=True)
    index = call(send_index_kernel, (QUAD, SHARED), [V, V, V])(
        elem_block.reshape(-1, LANES), shared_send.reshape(1, -1), token
    )
    count = 2 * CHIPS
    index = lax.ppermute(index, ("chip", "core"), [(i, (i - 1) % count) for i in range(count)])
    tile, block = call(own_index_kernel, ((ELEM_DEV // LANES, LANES),) * 2, [V, V])(index, shared_own.reshape(1, -1))
    inbox = lax.all_gather(inbox.reshape(CHIPS * ROWS, LANES), "core", tiled=True)
    return call(place_kernel, (QUAD, ELEM_DEV), [S] + [V] * 4)(
        core, inbox, elem_block.reshape(1, -1), tile.reshape(1, -1), block.reshape(1, -1)
    )


def solution(mesh):
    split = Mesh(mesh.devices.reshape(CHIPS, 2, -1), ("chip", "core", "rep"))
    spread = P(("rep", "chip", "core"))
    return jax.shard_map(
        per_device,
        mesh=split,
        in_specs=(spread, spread, P(), spread, spread, spread),
        out_specs=P(None, ("rep", "chip", "core")),
        check_vma=False,
    )
```

```python
import jax
import jax.numpy as jnp
from jax import lax
from jax.experimental import pallas as pl
from jax.experimental.pallas import tpu as pltpu
from jax.sharding import Mesh
from jax.sharding import PartitionSpec as P

LANES = 128
TILE_DEV = 128
ELEM_DEV = 1024
SHARED = 256
BLOCKS = 8
QUAD = 8
WIDTH = BLOCKS * QUAD
CHIPS = 64
ROWS = 4
FIRST = 42


def iota(shape, dim):
    return lax.broadcasted_iota(jnp.int32, shape, dim)


def split3(x):
    high = x.astype(jnp.bfloat16)
    rest = x - high.astype(jnp.float32)
    mid = rest.astype(jnp.bfloat16)
    low = (rest - mid.astype(jnp.float32)).astype(jnp.bfloat16)
    return high, mid, low


def dot(a, b, contract, **kw):
    return lax.dot_general(a, b, ((contract[:1], contract[1:]), ((), ())), preferred_element_type=jnp.float32, **kw)


def pack_kernel(tension_any, dest_any, restriction_any, out_ref, token_ref, tension_ref, dest_ref, restriction_ref, sems):
    pairs = ((restriction_any, restriction_ref), (dest_any, dest_ref), (tension_any, tension_ref))
    copies = [pltpu.make_async_copy(a, b, sems.at[i]) for i, (a, b) in enumerate(pairs)]
    for copy in copies:
        copy.start()
    copies[0].wait()
    wide = jnp.concatenate([restriction_ref[...]] * BLOCKS, axis=1)
    block = iota(wide.shape, 1) // (wide.shape[1] // BLOCKS)
    weight = jnp.concatenate([jnp.where(block == b, wide, 0.0) for b in range(BLOCKS)], axis=0)
    copies[1].wait()
    dest = dest_ref[...]
    target = dest >> 7
    position = (dest & (TILE_DEV - 1)).astype(jnp.float32)
    shape = (2 * CHIPS, TILE_DEV)
    row, lane = iota(shape, 0), iota(shape, 1)
    owner = 2 * ((row + FIRST) & (CHIPS - 1)) + (row >> 6)
    hit = jnp.broadcast_to(target, shape) == owner
    lane_f = lane.astype(jnp.float32)
    first = jnp.min(jnp.where(hit, lane_f, float(TILE_DEV)), axis=1, keepdims=True)
    one = lane_f == first
    two = jnp.logical_and(hit, lane_f != first)
    spread = jnp.broadcast_to(position, shape)
    where_one = jnp.max(jnp.where(one, spread, -1.0), axis=1, keepdims=True)
    where_two = jnp.max(jnp.where(two, spread, -1.0), axis=1, keepdims=True)
    pick = jnp.concatenate(
        [jnp.where(one, 1.0, 0.0).astype(jnp.bfloat16), jnp.where(two, 1.0, 0.0).astype(jnp.bfloat16)], axis=1
    )
    copies[2].wait()
    quad = dot(tension_ref[...], weight, (1, 1), precision=lax.Precision.HIGHEST)
    data = jnp.zeros(shape, jnp.float32)
    for part in split3(quad):
        nil = jnp.zeros_like(part)
        both = jnp.concatenate(
            [jnp.concatenate([part, nil], axis=1), jnp.concatenate([nil, part], axis=1)], axis=0
        )
        data = data + dot(pick, both, (1, 0))
    even, odd = data[:CHIPS], data[CHIPS:]

    def ahead(x):
        return jnp.concatenate([x[1:], x[:1]], axis=0)

    column = lane[:CHIPS]
    places = jnp.zeros((CHIPS, LANES), jnp.float32)
    firsts, seconds = where_one[:CHIPS], where_two[:CHIPS]
    columns = (firsts, seconds, where_one[CHIPS:], where_two[CHIPS:], ahead(firsts), ahead(seconds))
    for i, value in enumerate(columns):
        places = jnp.where(column == i, jnp.broadcast_to(value, places.shape), places)
    token_ref[...] = places[:8]
    for i, value in enumerate((even, odd, ahead(even), places)):
        out_ref[pl.ds(i, CHIPS, stride=ROWS), :] = value


def send_index_kernel(block_ref, send_ref, _, out_ref):
    block = block_ref[...]
    left = jnp.concatenate([block >> 3, block & 7], axis=0).astype(jnp.float32).astype(jnp.bfloat16)
    send = send_ref[...]
    shape = (LANES, SHARED)
    pick = jnp.where(iota(shape, 0) == jnp.broadcast_to(send & (LANES - 1), shape), 1.0, 0.0)
    rows = dot(left, pick.astype(jnp.bfloat16), (1, 0))
    shape = (ELEM_DEV // LANES, SHARED)
    high = iota(shape, 0) == jnp.broadcast_to(send >> 7, shape)
    tile = jnp.sum(jnp.where(high, rows[: shape[0]], 0.0), axis=0, keepdims=True)
    block = jnp.sum(jnp.where(high, rows[shape[0] :], 0.0), axis=0, keepdims=True)
    row = iota((QUAD, SHARED), 0)
    out_ref[...] = jnp.where(row == 0, jnp.broadcast_to(tile, row.shape), jnp.broadcast_to(block, row.shape))


def own_index_kernel(index_ref, own_ref, tile_ref, block_ref):
    own = own_ref[...]
    shape = (ELEM_DEV // LANES, SHARED)
    high = iota(shape, 0) == jnp.broadcast_to(own >> 7, shape)
    rows = [index_ref[0:1, :] + 1.0, index_ref[1:2, :]]
    left = jnp.concatenate([jnp.where(high, jnp.broadcast_to(row, shape), 0.0) for row in rows], axis=0)
    wide = (LANES, SHARED)
    pick = jnp.where(iota(wide, 0) == jnp.broadcast_to(own & (LANES - 1), wide), 1.0, 0.0)
    placed = dot(left.astype(jnp.bfloat16), pick.astype(jnp.bfloat16), (1, 1))
    tile_ref[...] = placed[: shape[0]] - 1.0
    block_ref[...] = placed[shape[0] :]


def gather(table, places, tile, block):
    turned = table.T
    left = jnp.concatenate(
        [jnp.concatenate([part[:WIDTH], part[WIDTH:]], axis=1) for part in split3(turned)], axis=0
    )
    shape = (TILE_DEV, tile.shape[1])
    wide = jnp.broadcast_to(tile, shape)
    pick = jnp.concatenate(
        [jnp.where(jnp.broadcast_to(place, shape) == wide, 1.0, 0.0).astype(jnp.bfloat16) for place in places], axis=0
    )
    tall = dot(left, pick, (1, 0))
    tall = tall[:WIDTH] + tall[WIDTH : 2 * WIDTH] + tall[2 * WIDTH :]
    which = jnp.broadcast_to(block, (QUAD, tile.shape[1]))
    out = jnp.zeros(which.shape, jnp.float32)
    for b in range(BLOCKS):
        out = jnp.where(which == float(b), tall[b * QUAD : (b + 1) * QUAD], out)
    return out


def place_kernel(core_ref, inbox_ref, block_ref, tile_ref, ghost_block_ref, out_ref):
    even_core = core_ref[0] == 0
    rows = [inbox_ref[pl.ds(i, 2 * CHIPS, stride=ROWS), :] for i in range(ROWS)]
    own = jnp.where(even_core, rows[0], rows[1])
    following = jnp.where(even_core, rows[1], rows[2])
    places = jnp.where(even_core, rows[3], pltpu.roll(rows[3], LANES - 2, 1))
    block = block_ref[...]
    mine = gather(
        own,
        (places[:, 0:1], places[:, 1:2]),
        (block >> 3).astype(jnp.float32),
        (block & 7).astype(jnp.float32),
    )
    tile = tile_ref[...]
    ghost = gather(following, (places[:, 2:3], places[:, 3:4]), tile, ghost_block_ref[...])
    shared = jnp.broadcast_to(tile, ghost.shape) >= 0.0
    out_ref[...] = jnp.where(shared, 0.5 * (mine + ghost), mine)


def call(kernel, shapes, spaces, scratch=(), limit=4):
    return pl.pallas_call(
        kernel,
        out_shape=jax.tree.map(lambda s: jax.ShapeDtypeStruct(s, jnp.float32), shapes, is_leaf=lambda s: isinstance(s[0], int)),
        in_specs=[pl.BlockSpec(memory_space=space) for space in spaces],
        scratch_shapes=scratch,
        compiler_params=pltpu.CompilerParams(vmem_limit_bytes=limit << 20),
        name=kernel.__name__,
    )


def per_device(tension, tile_dest, restriction, elem_block, shared_own, shared_send):
    V, S = pltpu.VMEM, pltpu.SMEM
    core = lax.axis_index("core").reshape(1)
    inputs = (tension, tile_dest.reshape(1, -1), restriction)
    scratch = [V(x.shape, x.dtype) for x in inputs] + [pltpu.SemaphoreType.DMA((3,))]
    outbox, token = call(pack_kernel, ((CHIPS * ROWS, LANES), (8, LANES)), [pl.ANY] * 3, scratch, 60)(*inputs)
    groups = [[2 * ((FIRST + i) % CHIPS) + c for i in range(CHIPS)] for c in range(2)]
    inbox = lax.all_to_all(
        outbox.reshape(CHIPS, ROWS, LANES), ("chip", "core"), 0, 0, axis_index_groups=groups, tiled=True
    )
    index = call(send_index_kernel, (QUAD, SHARED), [V, V, V])(
        elem_block.reshape(-1, LANES), shared_send.reshape(1, -1), token
    )
    count = 2 * CHIPS
    index = lax.ppermute(index, ("chip", "core"), [(i, (i - 1) % count) for i in range(count)])
    tile, block = call(own_index_kernel, ((ELEM_DEV // LANES, LANES),) * 2, [V, V])(index, shared_own.reshape(1, -1))
    inbox = lax.all_gather(inbox.reshape(CHIPS * ROWS, LANES), "core", tiled=True)
    return call(place_kernel, (QUAD, ELEM_DEV), [S] + [V] * 4)(
        core, inbox, elem_block.reshape(1, -1), tile.reshape(1, -1), block.reshape(1, -1)
    )


def solution(mesh):
    split = Mesh(mesh.devices.reshape(CHIPS, 2, -1), ("chip", "core", "rep"))
    spread = P(("rep", "chip", "core"))
    return jax.shard_map(
        per_device,
        mesh=split,
        in_specs=(spread, spread, P(), spread, spread, spread),
        out_specs=P(None, ("rep", "chip", "core")),
        check_vma=False,
    )
```

```python
import jax
import jax.numpy as jnp
from jax import lax
from jax.experimental import pallas as pl
from jax.experimental.pallas import tpu as pltpu
from jax.sharding import Mesh
from jax.sharding import PartitionSpec as P

LANES = 128
TILE_DEV = 128
ELEM_DEV = 1024
SHARED = 256
BLOCKS = 8
QUAD = 8
WIDTH = BLOCKS * QUAD
CHIPS = 64
ROWS = 4
FIRST = 42
RING = 16


def iota(shape, dim):
    return lax.broadcasted_iota(jnp.int32, shape, dim)


def split3(x):
    high = x.astype(jnp.bfloat16)
    rest = x - high.astype(jnp.float32)
    mid = rest.astype(jnp.bfloat16)
    low = (rest - mid.astype(jnp.float32)).astype(jnp.bfloat16)
    return high, mid, low


def dot(a, b, contract, **kw):
    return lax.dot_general(a, b, ((contract[:1], contract[1:]), ((), ())), preferred_element_type=jnp.float32, **kw)


def pack_kernel(tension_any, dest_any, restriction_any, out_ref, token_ref, tension_ref, dest_ref, restriction_ref, sems):
    pairs = ((restriction_any, restriction_ref), (dest_any, dest_ref), (tension_any, tension_ref))
    copies = [pltpu.make_async_copy(a, b, sems.at[i]) for i, (a, b) in enumerate(pairs)]
    for copy in copies:
        copy.start()
    copies[0].wait()
    wide = jnp.concatenate([restriction_ref[...]] * BLOCKS, axis=1)
    block = iota(wide.shape, 1) // (wide.shape[1] // BLOCKS)
    weight = jnp.concatenate([jnp.where(block == b, wide, 0.0) for b in range(BLOCKS)], axis=0)
    copies[1].wait()
    dest = dest_ref[...]
    target = dest >> 7
    position = (dest & (TILE_DEV - 1)).astype(jnp.float32)
    shape = (2 * CHIPS, TILE_DEV)
    row, lane = iota(shape, 0), iota(shape, 1)
    owner = 2 * ((row + FIRST) & (CHIPS - 1)) + (row >> 6)
    hit = jnp.broadcast_to(target, shape) == owner
    lane_f = lane.astype(jnp.float32)
    first = jnp.min(jnp.where(hit, lane_f, float(TILE_DEV)), axis=1, keepdims=True)
    one = lane_f == first
    two = jnp.logical_and(hit, lane_f != first)
    spread = jnp.broadcast_to(position, shape)
    where_one = jnp.max(jnp.where(one, spread, -1.0), axis=1, keepdims=True)
    where_two = jnp.max(jnp.where(two, spread, -1.0), axis=1, keepdims=True)
    pick = jnp.concatenate(
        [jnp.where(one, 1.0, 0.0).astype(jnp.bfloat16), jnp.where(two, 1.0, 0.0).astype(jnp.bfloat16)], axis=1
    )
    copies[2].wait()
    quad = dot(tension_ref[...], weight, (1, 1), precision=lax.Precision.HIGHEST)
    data = jnp.zeros(shape, jnp.float32)
    for part in split3(quad):
        nil = jnp.zeros_like(part)
        both = jnp.concatenate(
            [jnp.concatenate([part, nil], axis=1), jnp.concatenate([nil, part], axis=1)], axis=0
        )
        data = data + dot(pick, both, (1, 0))
    even, odd = data[:CHIPS], data[CHIPS:]

    def ahead(x):
        return jnp.concatenate([x[1:], x[:1]], axis=0)

    column = lane[:CHIPS]
    places = jnp.zeros((CHIPS, LANES), jnp.float32)
    firsts, seconds = where_one[:CHIPS], where_two[:CHIPS]
    columns = (firsts, seconds, where_one[CHIPS:], where_two[CHIPS:], ahead(firsts), ahead(seconds))
    for i, value in enumerate(columns):
        places = jnp.where(column == i, jnp.broadcast_to(value, places.shape), places)
    token_ref[...] = places[:8]
    for i, value in enumerate((even, odd, ahead(even), places)):
        out_ref[pl.ds(i, CHIPS, stride=ROWS), :] = value


def send_index_kernel(block_ref, send_ref, _, out_ref):
    block = block_ref[...]
    left = jnp.concatenate([block >> 3, block & 7], axis=0).astype(jnp.float32).astype(jnp.bfloat16)
    send = send_ref[...]
    shape = (LANES, SHARED)
    pick = jnp.where(iota(shape, 0) == jnp.broadcast_to(send & (LANES - 1), shape), 1.0, 0.0)
    rows = dot(left, pick.astype(jnp.bfloat16), (1, 0))
    shape = (ELEM_DEV // LANES, SHARED)
    high = iota(shape, 0) == jnp.broadcast_to(send >> 7, shape)
    tile = jnp.sum(jnp.where(high, rows[: shape[0]], 0.0), axis=0, keepdims=True)
    block = jnp.sum(jnp.where(high, rows[shape[0] :], 0.0), axis=0, keepdims=True)
    row = iota((QUAD, SHARED), 0)
    out_ref[...] = jnp.where(row == 0, jnp.broadcast_to(tile, row.shape), jnp.broadcast_to(block, row.shape))


def own_index_kernel(index_ref, own_ref, tile_ref, block_ref):
    own = own_ref[...]
    shape = (ELEM_DEV // LANES, SHARED)
    high = iota(shape, 0) == jnp.broadcast_to(own >> 7, shape)
    rows = [index_ref[0:1, :] + 1.0, index_ref[1:2, :]]
    left = jnp.concatenate([jnp.where(high, jnp.broadcast_to(row, shape), 0.0) for row in rows], axis=0)
    wide = (LANES, SHARED)
    pick = jnp.where(iota(wide, 0) == jnp.broadcast_to(own & (LANES - 1), wide), 1.0, 0.0)
    placed = dot(left.astype(jnp.bfloat16), pick.astype(jnp.bfloat16), (1, 1))
    tile_ref[...] = placed[: shape[0]] - 1.0
    block_ref[...] = placed[shape[0] :]


def gather(table, places, tile, block):
    turned = table.T
    left = jnp.concatenate(
        [jnp.concatenate([part[:WIDTH], part[WIDTH:]], axis=1) for part in split3(turned)], axis=0
    )
    shape = (TILE_DEV, tile.shape[1])
    wide = jnp.broadcast_to(tile, shape)
    pick = jnp.concatenate(
        [jnp.where(jnp.broadcast_to(place, shape) == wide, 1.0, 0.0).astype(jnp.bfloat16) for place in places], axis=0
    )
    tall = dot(left, pick, (1, 0))
    tall = tall[:WIDTH] + tall[WIDTH : 2 * WIDTH] + tall[2 * WIDTH :]
    which = jnp.broadcast_to(block, (QUAD, tile.shape[1]))
    out = jnp.zeros(which.shape, jnp.float32)
    for b in range(BLOCKS):
        out = jnp.where(which == float(b), tall[b * QUAD : (b + 1) * QUAD], out)
    return out


def place_kernel(core_ref, inbox_ref, block_ref, tile_ref, ghost_block_ref, out_ref):
    even_core = core_ref[0] == 0
    rows = [inbox_ref[pl.ds(i, 2 * CHIPS, stride=ROWS), :] for i in range(ROWS)]
    own = jnp.where(even_core, rows[0], rows[1])
    following = jnp.where(even_core, rows[1], rows[2])
    places = jnp.where(even_core, rows[3], pltpu.roll(rows[3], LANES - 2, 1))
    block = block_ref[...]
    mine = gather(
        own,
        (places[:, 0:1], places[:, 1:2]),
        (block >> 3).astype(jnp.float32),
        (block & 7).astype(jnp.float32),
    )
    tile = tile_ref[...]
    ghost = gather(following, (places[:, 2:3], places[:, 3:4]), tile, ghost_block_ref[...])
    shared = jnp.broadcast_to(tile, ghost.shape) >= 0.0
    out_ref[...] = jnp.where(shared, 0.5 * (mine + ghost), mine)


def call(kernel, shapes, spaces, scratch=(), limit=4):
    return pl.pallas_call(
        kernel,
        out_shape=jax.tree.map(lambda s: jax.ShapeDtypeStruct(s, jnp.float32), shapes, is_leaf=lambda s: isinstance(s[0], int)),
        in_specs=[pl.BlockSpec(memory_space=space) for space in spaces],
        scratch_shapes=scratch,
        compiler_params=pltpu.CompilerParams(vmem_limit_bytes=limit << 20),
        name=kernel.__name__,
    )


def per_device(tension, tile_dest, restriction, elem_block, shared_own, shared_send):
    V, S = pltpu.VMEM, pltpu.SMEM
    core = lax.axis_index("core").reshape(1)
    inputs = (tension, tile_dest.reshape(1, -1), restriction)
    scratch = [V(x.shape, x.dtype) for x in inputs] + [pltpu.SemaphoreType.DMA((3,))]
    outbox, token = call(pack_kernel, ((CHIPS * ROWS, LANES), (8, LANES)), [pl.ANY] * 3, scratch, 60)(*inputs)
    order = [(FIRST + i) % CHIPS for i in range(CHIPS)]
    groups = [[2 * chip + (c ^ (chip % RING == 0)) for chip in order] for c in range(2)]
    inbox = lax.all_to_all(
        outbox.reshape(CHIPS, ROWS, LANES), ("chip", "core"), 0, 0, axis_index_groups=groups, tiled=True
    )
    index = call(send_index_kernel, (QUAD, SHARED), [V, V, V])(
        elem_block.reshape(-1, LANES), shared_send.reshape(1, -1), token
    )
    count = 2 * CHIPS
    index = lax.ppermute(index, ("chip", "core"), [(i, (i - 1) % count) for i in range(count)])
    tile, block = call(own_index_kernel, ((ELEM_DEV // LANES, LANES),) * 2, [V, V])(index, shared_own.reshape(1, -1))
    inbox = lax.all_gather(inbox.reshape(CHIPS * ROWS, LANES), "core", tiled=True)
    return call(place_kernel, (QUAD, ELEM_DEV), [S] + [V] * 4)(
        core, inbox, elem_block.reshape(1, -1), tile.reshape(1, -1), block.reshape(1, -1)
    )


def solution(mesh):
    split = Mesh(mesh.devices.reshape(CHIPS, 2, -1), ("chip", "core", "rep"))
    spread = P(("rep", "chip", "core"))
    return jax.shard_map(
        per_device,
        mesh=split,
        in_specs=(spread, spread, P(), spread, spread, spread),
        out_specs=P(None, ("rep", "chip", "core")),
        check_vma=False,
    )
```

```python
import jax
import jax.numpy as jnp
from jax import lax
from jax.experimental import pallas as pl
from jax.experimental.pallas import tpu as pltpu
from jax.sharding import Mesh
from jax.sharding import PartitionSpec as P

LANES = 128
TILE_DEV = 128
ELEM_DEV = 1024
SHARED = 256
BLOCKS = 8
QUAD = 8
WIDTH = BLOCKS * QUAD
CHIPS = 64
ROWS = 4
FIRST = 42
RING = 16
STRIDE = 3


def iota(shape, dim):
    return lax.broadcasted_iota(jnp.int32, shape, dim)


def split3(x):
    high = x.astype(jnp.bfloat16)
    rest = x - high.astype(jnp.float32)
    mid = rest.astype(jnp.bfloat16)
    low = (rest - mid.astype(jnp.float32)).astype(jnp.bfloat16)
    return high, mid, low


def dot(a, b, contract, **kw):
    return lax.dot_general(a, b, ((contract[:1], contract[1:]), ((), ())), preferred_element_type=jnp.float32, **kw)


def pack_kernel(tension_any, dest_any, restriction_any, out_ref, token_ref, tension_ref, dest_ref, restriction_ref, sems):
    pairs = ((restriction_any, restriction_ref), (dest_any, dest_ref), (tension_any, tension_ref))
    copies = [pltpu.make_async_copy(a, b, sems.at[i]) for i, (a, b) in enumerate(pairs)]
    for copy in copies:
        copy.start()
    copies[0].wait()
    wide = jnp.concatenate([restriction_ref[...]] * BLOCKS, axis=1)
    block = iota(wide.shape, 1) // (wide.shape[1] // BLOCKS)
    weight = jnp.concatenate([jnp.where(block == b, wide, 0.0) for b in range(BLOCKS)], axis=0)
    copies[1].wait()
    dest = dest_ref[...]
    target = dest >> 7
    position = (dest & (TILE_DEV - 1)).astype(jnp.float32)
    shape = (2 * CHIPS, TILE_DEV)
    row, lane = iota(shape, 0), iota(shape, 1)
    owner = 2 * ((STRIDE * row + FIRST) & (CHIPS - 1)) + (row >> 6)
    hit = jnp.broadcast_to(target, shape) == owner
    lane_f = lane.astype(jnp.float32)
    first = jnp.min(jnp.where(hit, lane_f, float(TILE_DEV)), axis=1, keepdims=True)
    one = lane_f == first
    two = jnp.logical_and(hit, lane_f != first)
    spread = jnp.broadcast_to(position, shape)
    where_one = jnp.max(jnp.where(one, spread, -1.0), axis=1, keepdims=True)
    where_two = jnp.max(jnp.where(two, spread, -1.0), axis=1, keepdims=True)
    pick = jnp.concatenate(
        [jnp.where(one, 1.0, 0.0).astype(jnp.bfloat16), jnp.where(two, 1.0, 0.0).astype(jnp.bfloat16)], axis=1
    )
    copies[2].wait()
    quad = dot(tension_ref[...], weight, (1, 1), precision=lax.Precision.HIGHEST)
    data = jnp.zeros(shape, jnp.float32)
    for part in split3(quad):
        nil = jnp.zeros_like(part)
        both = jnp.concatenate(
            [jnp.concatenate([part, nil], axis=1), jnp.concatenate([nil, part], axis=1)], axis=0
        )
        data = data + dot(pick, both, (1, 0))
    even, odd = data[:CHIPS], data[CHIPS:]

    def ahead(x):
        step = pow(STRIDE, -1, CHIPS)
        return jnp.concatenate([x[step:], x[:step]], axis=0)

    column = lane[:CHIPS]
    places = jnp.zeros((CHIPS, LANES), jnp.float32)
    firsts, seconds = where_one[:CHIPS], where_two[:CHIPS]
    columns = (firsts, seconds, where_one[CHIPS:], where_two[CHIPS:], ahead(firsts), ahead(seconds))
    for i, value in enumerate(columns):
        places = jnp.where(column == i, jnp.broadcast_to(value, places.shape), places)
    token_ref[...] = places[:8]
    for i, value in enumerate((even, odd, ahead(even), places)):
        out_ref[pl.ds(i, CHIPS, stride=ROWS), :] = value


def send_index_kernel(block_ref, send_ref, _, out_ref):
    block = block_ref[...]
    left = jnp.concatenate([block >> 3, block & 7], axis=0).astype(jnp.float32).astype(jnp.bfloat16)
    send = send_ref[...]
    shape = (LANES, SHARED)
    pick = jnp.where(iota(shape, 0) == jnp.broadcast_to(send & (LANES - 1), shape), 1.0, 0.0)
    rows = dot(left, pick.astype(jnp.bfloat16), (1, 0))
    shape = (ELEM_DEV // LANES, SHARED)
    high = iota(shape, 0) == jnp.broadcast_to(send >> 7, shape)
    tile = jnp.sum(jnp.where(high, rows[: shape[0]], 0.0), axis=0, keepdims=True)
    block = jnp.sum(jnp.where(high, rows[shape[0] :], 0.0), axis=0, keepdims=True)
    row = iota((QUAD, SHARED), 0)
    out_ref[...] = jnp.where(row == 0, jnp.broadcast_to(tile, row.shape), jnp.broadcast_to(block, row.shape))


def own_index_kernel(index_ref, own_ref, tile_ref, block_ref):
    own = own_ref[...]
    shape = (ELEM_DEV // LANES, SHARED)
    high = iota(shape, 0) == jnp.broadcast_to(own >> 7, shape)
    rows = [index_ref[0:1, :] + 1.0, index_ref[1:2, :]]
    left = jnp.concatenate([jnp.where(high, jnp.broadcast_to(row, shape), 0.0) for row in rows], axis=0)
    wide = (LANES, SHARED)
    pick = jnp.where(iota(wide, 0) == jnp.broadcast_to(own & (LANES - 1), wide), 1.0, 0.0)
    placed = dot(left.astype(jnp.bfloat16), pick.astype(jnp.bfloat16), (1, 1))
    tile_ref[...] = placed[: shape[0]] - 1.0
    block_ref[...] = placed[shape[0] :]


def gather(table, places, tile, block):
    turned = table.T
    left = jnp.concatenate(
        [jnp.concatenate([part[:WIDTH], part[WIDTH:]], axis=1) for part in split3(turned)], axis=0
    )
    shape = (TILE_DEV, tile.shape[1])
    wide = jnp.broadcast_to(tile, shape)
    pick = jnp.concatenate(
        [jnp.where(jnp.broadcast_to(place, shape) == wide, 1.0, 0.0).astype(jnp.bfloat16) for place in places], axis=0
    )
    tall = dot(left, pick, (1, 0))
    tall = tall[:WIDTH] + tall[WIDTH : 2 * WIDTH] + tall[2 * WIDTH :]
    which = jnp.broadcast_to(block, (QUAD, tile.shape[1]))
    out = jnp.zeros(which.shape, jnp.float32)
    for b in range(BLOCKS):
        out = jnp.where(which == float(b), tall[b * QUAD : (b + 1) * QUAD], out)
    return out


def place_kernel(core_ref, inbox_ref, block_ref, tile_ref, ghost_block_ref, out_ref):
    even_core = core_ref[0] == 0
    rows = [inbox_ref[pl.ds(i, 2 * CHIPS, stride=ROWS), :] for i in range(ROWS)]
    own = jnp.where(even_core, rows[0], rows[1])
    following = jnp.where(even_core, rows[1], rows[2])
    places = jnp.where(even_core, rows[3], pltpu.roll(rows[3], LANES - 2, 1))
    block = block_ref[...]
    mine = gather(
        own,
        (places[:, 0:1], places[:, 1:2]),
        (block >> 3).astype(jnp.float32),
        (block & 7).astype(jnp.float32),
    )
    tile = tile_ref[...]
    ghost = gather(following, (places[:, 2:3], places[:, 3:4]), tile, ghost_block_ref[...])
    shared = jnp.broadcast_to(tile, ghost.shape) >= 0.0
    out_ref[...] = jnp.where(shared, 0.5 * (mine + ghost), mine)


def call(kernel, shapes, spaces, scratch=(), limit=4):
    return pl.pallas_call(
        kernel,
        out_shape=jax.tree.map(lambda s: jax.ShapeDtypeStruct(s, jnp.float32), shapes, is_leaf=lambda s: isinstance(s[0], int)),
        in_specs=[pl.BlockSpec(memory_space=space) for space in spaces],
        scratch_shapes=scratch,
        compiler_params=pltpu.CompilerParams(vmem_limit_bytes=limit << 20),
        name=kernel.__name__,
    )


def per_device(tension, tile_dest, restriction, elem_block, shared_own, shared_send):
    V, S = pltpu.VMEM, pltpu.SMEM
    core = lax.axis_index("core").reshape(1)
    inputs = (tension, tile_dest.reshape(1, -1), restriction)
    scratch = [V(x.shape, x.dtype) for x in inputs] + [pltpu.SemaphoreType.DMA((3,))]
    outbox, token = call(pack_kernel, ((CHIPS * ROWS, LANES), (8, LANES)), [pl.ANY] * 3, scratch, 60)(*inputs)
    order = [(FIRST + STRIDE * i) % CHIPS for i in range(CHIPS)]
    groups = [[2 * chip + (c ^ (chip % RING == 0)) for chip in order] for c in range(2)]
    inbox = lax.all_to_all(
        outbox.reshape(CHIPS, ROWS, LANES), ("chip", "core"), 0, 0, axis_index_groups=groups, tiled=True
    )
    index = call(send_index_kernel, (QUAD, SHARED), [V, V, V])(
        elem_block.reshape(-1, LANES), shared_send.reshape(1, -1), token
    )
    count = 2 * CHIPS
    index = lax.ppermute(index, ("chip", "core"), [(i, (i - 1) % count) for i in range(count)])
    tile, block = call(own_index_kernel, ((ELEM_DEV // LANES, LANES),) * 2, [V, V])(index, shared_own.reshape(1, -1))
    inbox = lax.all_gather(inbox.reshape(CHIPS * ROWS, LANES), "core", tiled=True)
    return call(place_kernel, (QUAD, ELEM_DEV), [S] + [V] * 4)(
        core, inbox, elem_block.reshape(1, -1), tile.reshape(1, -1), block.reshape(1, -1)
    )


def solution(mesh):
    split = Mesh(mesh.devices.reshape(CHIPS, 2, -1), ("chip", "core", "rep"))
    spread = P(("rep", "chip", "core"))
    return jax.shard_map(
        per_device,
        mesh=split,
        in_specs=(spread, spread, P(), spread, spread, spread),
        out_specs=P(None, ("rep", "chip", "core")),
        check_vma=False,
    )
```

```python
import jax
import jax.numpy as jnp
from jax import lax
from jax.experimental import pallas as pl
from jax.experimental.pallas import tpu as pltpu
from jax.sharding import Mesh
from jax.sharding import PartitionSpec as P

LANES = 128
TILE_DEV = 128
ELEM_DEV = 1024
SHARED = 256
BLOCKS = 8
QUAD = 8
WIDTH = BLOCKS * QUAD
CHIPS = 64
ROWS = 4
FIRST = 42
RING = 16
STRIDE = 3


def iota(shape, dim):
    return lax.broadcasted_iota(jnp.int32, shape, dim)


def split3(x):
    high = x.astype(jnp.bfloat16)
    rest = x - high.astype(jnp.float32)
    mid = rest.astype(jnp.bfloat16)
    low = (rest - mid.astype(jnp.float32)).astype(jnp.bfloat16)
    return high, mid, low


def dot(a, b, contract, **kw):
    return lax.dot_general(a, b, ((contract[:1], contract[1:]), ((), ())), preferred_element_type=jnp.float32, **kw)


def pack_kernel(tension_any, dest_any, restriction_any, out_ref, token_ref, tension_ref, dest_ref, restriction_ref, sems):
    pairs = ((restriction_any, restriction_ref), (dest_any, dest_ref), (tension_any, tension_ref))
    copies = [pltpu.make_async_copy(a, b, sems.at[i]) for i, (a, b) in enumerate(pairs)]
    for copy in copies:
        copy.start()
    copies[0].wait()
    wide = jnp.concatenate([restriction_ref[...]] * BLOCKS, axis=1)
    block = iota(wide.shape, 1) // (wide.shape[1] // BLOCKS)
    weight = jnp.concatenate([jnp.where(block == b, wide, 0.0) for b in range(BLOCKS)], axis=0)
    copies[1].wait()
    dest = dest_ref[...]
    target = dest >> 7
    position = (dest & (TILE_DEV - 1)).astype(jnp.float32)
    shape = (2 * CHIPS, TILE_DEV)
    row, lane = iota(shape, 0), iota(shape, 1)
    owner = 2 * ((STRIDE * row + FIRST) & (CHIPS - 1)) + (row >> 6)
    hit = jnp.broadcast_to(target, shape) == owner
    lane_f = lane.astype(jnp.float32)
    first = jnp.min(jnp.where(hit, lane_f, float(TILE_DEV)), axis=1, keepdims=True)
    one = lane_f == first
    two = jnp.logical_and(hit, lane_f != first)
    spread = jnp.broadcast_to(position, shape)
    where_one = jnp.max(jnp.where(one, spread, -1.0), axis=1, keepdims=True)
    where_two = jnp.max(jnp.where(two, spread, -1.0), axis=1, keepdims=True)
    pick = jnp.concatenate(
        [jnp.where(one, 1.0, 0.0).astype(jnp.bfloat16), jnp.where(two, 1.0, 0.0).astype(jnp.bfloat16)], axis=1
    )
    copies[2].wait()
    quad = dot(tension_ref[...], weight, (1, 1), precision=lax.Precision.HIGHEST)
    data = jnp.zeros(shape, jnp.float32)
    for part in split3(quad):
        nil = jnp.zeros_like(part)
        both = jnp.concatenate(
            [jnp.concatenate([part, nil], axis=1), jnp.concatenate([nil, part], axis=1)], axis=0
        )
        data = data + dot(pick, both, (1, 0))
    even, odd = data[:CHIPS], data[CHIPS:]

    def ahead(x):
        step = pow(STRIDE, -1, CHIPS)
        return jnp.concatenate([x[step:], x[:step]], axis=0)

    column = lane[:CHIPS]
    places = jnp.zeros((CHIPS, LANES), jnp.float32)
    firsts, seconds = where_one[:CHIPS], where_two[:CHIPS]
    columns = (firsts, seconds, where_one[CHIPS:], where_two[CHIPS:], ahead(firsts), ahead(seconds))
    for i, value in enumerate(columns):
        places = jnp.where(column == i, jnp.broadcast_to(value, places.shape), places)
    token_ref[...] = places[:8]
    for i, value in enumerate((even, odd, ahead(even), places)):
        out_ref[pl.ds(i, CHIPS, stride=ROWS), :] = value


def send_index_kernel(block_ref, send_ref, _, out_ref):
    block = block_ref[...]
    left = jnp.concatenate([block >> 3, block & 7], axis=0).astype(jnp.float32).astype(jnp.bfloat16)
    send = send_ref[...]
    shape = (LANES, SHARED)
    pick = jnp.where(iota(shape, 0) == jnp.broadcast_to(send & (LANES - 1), shape), 1.0, 0.0)
    rows = dot(left, pick.astype(jnp.bfloat16), (1, 0))
    shape = (ELEM_DEV // LANES, SHARED)
    high = iota(shape, 0) == jnp.broadcast_to(send >> 7, shape)
    tile = jnp.sum(jnp.where(high, rows[: shape[0]], 0.0), axis=0, keepdims=True)
    block = jnp.sum(jnp.where(high, rows[shape[0] :], 0.0), axis=0, keepdims=True)
    row = iota((QUAD, SHARED), 0)
    out_ref[...] = jnp.where(row == 0, jnp.broadcast_to(tile, row.shape), jnp.broadcast_to(block, row.shape))


def own_index_kernel(index_ref, own_ref, tile_ref, block_ref):
    own = own_ref[...]
    shape = (ELEM_DEV // LANES, SHARED)
    high = iota(shape, 0) == jnp.broadcast_to(own >> 7, shape)
    rows = [index_ref[0:1, :] + 1.0, index_ref[1:2, :]]
    left = jnp.concatenate([jnp.where(high, jnp.broadcast_to(row, shape), 0.0) for row in rows], axis=0)
    wide = (LANES, SHARED)
    pick = jnp.where(iota(wide, 0) == jnp.broadcast_to(own & (LANES - 1), wide), 1.0, 0.0)
    placed = dot(left.astype(jnp.bfloat16), pick.astype(jnp.bfloat16), (1, 1))
    tile_ref[...] = placed[: shape[0]] - 1.0
    block_ref[...] = placed[shape[0] :]


def gather(table, places, tile, block):
    turned = table.T
    left = jnp.concatenate(
        [jnp.concatenate([part[:WIDTH], part[WIDTH:]], axis=1) for part in split3(turned)], axis=0
    )
    shape = (TILE_DEV, tile.shape[1])
    wide = jnp.broadcast_to(tile.astype(jnp.bfloat16), shape)
    one, nil = jnp.ones(shape, jnp.bfloat16), jnp.zeros(shape, jnp.bfloat16)
    pick = jnp.concatenate(
        [jnp.where(jnp.concatenate([jnp.broadcast_to(place, (TILE_DEV, LANES)).astype(jnp.bfloat16)] * (shape[1] // LANES), axis=1) == wide, one, nil) for place in places], axis=0
    )
    tall = dot(left, pick, (1, 0))
    tall = tall[:WIDTH] + tall[WIDTH : 2 * WIDTH] + tall[2 * WIDTH :]
    which = jnp.broadcast_to(block, (QUAD, tile.shape[1]))
    out = jnp.zeros(which.shape, jnp.float32)
    for b in range(BLOCKS):
        out = jnp.where(which == float(b), tall[b * QUAD : (b + 1) * QUAD], out)
    return out


def place_kernel(core_ref, inbox_ref, block_ref, tile_ref, ghost_block_ref, out_ref):
    even_core = core_ref[0] == 0
    rows = [inbox_ref[pl.ds(i, 2 * CHIPS, stride=ROWS), :] for i in range(ROWS)]
    own = jnp.where(even_core, rows[0], rows[1])
    following = jnp.where(even_core, rows[1], rows[2])
    places = jnp.where(even_core, rows[3], pltpu.roll(rows[3], LANES - 2, 1))
    block = block_ref[...]
    mine = gather(
        own,
        (places[:, 0:1], places[:, 1:2]),
        (block >> 3).astype(jnp.float32),
        (block & 7).astype(jnp.float32),
    )
    tile = tile_ref[...]
    ghost = gather(following, (places[:, 2:3], places[:, 3:4]), tile, ghost_block_ref[...])
    shared = jnp.broadcast_to(tile, ghost.shape) >= 0.0
    out_ref[...] = jnp.where(shared, 0.5 * (mine + ghost), mine)


def call(kernel, shapes, spaces, scratch=(), limit=4):
    return pl.pallas_call(
        kernel,
        out_shape=jax.tree.map(lambda s: jax.ShapeDtypeStruct(s, jnp.float32), shapes, is_leaf=lambda s: isinstance(s[0], int)),
        in_specs=[pl.BlockSpec(memory_space=space) for space in spaces],
        scratch_shapes=scratch,
        compiler_params=pltpu.CompilerParams(vmem_limit_bytes=limit << 20),
        name=kernel.__name__,
    )


def per_device(tension, tile_dest, restriction, elem_block, shared_own, shared_send):
    V, S = pltpu.VMEM, pltpu.SMEM
    core = lax.axis_index("core").reshape(1)
    inputs = (tension, tile_dest.reshape(1, -1), restriction)
    scratch = [V(x.shape, x.dtype) for x in inputs] + [pltpu.SemaphoreType.DMA((3,))]
    outbox, token = call(pack_kernel, ((CHIPS * ROWS, LANES), (8, LANES)), [pl.ANY] * 3, scratch, 60)(*inputs)
    order = [(FIRST + STRIDE * i) % CHIPS for i in range(CHIPS)]
    groups = [[2 * chip + (c ^ (chip % RING == 0)) for chip in order] for c in range(2)]
    inbox = lax.all_to_all(
        outbox.reshape(CHIPS, ROWS, LANES), ("chip", "core"), 0, 0, axis_index_groups=groups, tiled=True
    )
    index = call(send_index_kernel, (QUAD, SHARED), [V, V, V])(
        elem_block.reshape(-1, LANES), shared_send.reshape(1, -1), token
    )
    count = 2 * CHIPS
    index = lax.ppermute(index, ("chip", "core"), [(i, (i - 1) % count) for i in range(count)])
    tile, block = call(own_index_kernel, ((ELEM_DEV // LANES, LANES),) * 2, [V, V])(index, shared_own.reshape(1, -1))
    inbox = lax.all_gather(inbox.reshape(CHIPS * ROWS, LANES), "core", tiled=True)
    return call(place_kernel, (QUAD, ELEM_DEV), [S] + [V] * 4)(
        core, inbox, elem_block.reshape(1, -1), tile.reshape(1, -1), block.reshape(1, -1)
    )


def solution(mesh):
    split = Mesh(mesh.devices.reshape(CHIPS, 2, -1), ("chip", "core", "rep"))
    spread = P(("rep", "chip", "core"))
    return jax.shard_map(
        per_device,
        mesh=split,
        in_specs=(spread, spread, P(), spread, spread, spread),
        out_specs=P(None, ("rep", "chip", "core")),
        check_vma=False,
    )
```
